32 devices in a mesh: docs: 2 (over x), seq: 16 (over z, y, core).
Axes of the slice: x: 2, y: 2, z: 4, core: 2. Of those that a mesh axis runs over, the one named last changes fastest.
Arguments:
- hidden_in: bfloat16 [8192, 4096], P(('docs', 'seq')), parts along dimension 0, may hold values from -6 to 6
- mix_norm_gain: float32 [4096], replicated, may hold values from 0.5 to 1.5
- ssm_proj: bfloat16 [4096, 64], replicated, may hold values from -0.09375 to 0.09375
- dt_bias: float32 [32], replicated, may hold values from -1 to 1
- decay_rate: float32 [32], replicated, may hold values from 4.8828124e-06 to 0.05
- mixer_gain: float32 [4096], replicated, may hold values from 0.5 to 1.5
- ffn_norm_gain: float32 [4096], replicated, may hold values from 0.5 to 1.5
- router: bfloat16 [4096, 16], replicated, may hold values from -0.09375 to 0.09375
- routes: int32 [8192, 2], P(('docs', 'seq')), parts along dimension 0, may hold values from 0 to 15, as said below
- w_gate: bfloat16 [4096, 3584], P(None, 'seq'), may hold values from -0.09375 to 0.09375
- w_up: bfloat16 [4096, 3584], P(None, 'seq'), may hold values from -0.09375 to 0.09375
- w_down: bfloat16 [3584, 4096], P('seq'), may hold values from -0.09375 to 0.09375
Outputs:
- block_out: bfloat16 [8192, 4096], P(('docs', 'seq')), parts along dimension 0
The draws below stay inside these ranges and needn't reach their ends.
There are 2 independent parts, one for each index of `docs`. The reference program is written for one: setup_inputs(seed, part) draws one part's arguments, and reference() takes and returns one part's arrays. A program takes and returns all parts, laid end to end along the dimension named above; an argument that names none is the same for every part. Nothing has to cross between parts.
Inputs may be any that keep to these rules, and one draw needn't show every extreme that they name: `routes`: each token names two different experts. Among the 256 tokens of one device at most 16 name expert 0, and on some device exactly 16 do.
All inputs are finite; a program needn't handle non-finite values.
Results may differ from the reference program's by a relative error of at most 0.0056.
Values may be sent and summed in bfloat16 or wider, within the bound.
A program may use at most 128 MiB of HBM per device.

```python
import math
import jax
import jax.numpy as jnp
from jax import lax

D = 4096
EXPERTS = 16
STATE = 16
HEADS = 32
FF = 3584
TOK_DEV = 256
SPAN = 128
CAP = 16
TOKENS = 4096


def draw_routes(key, part):
    blocks = TOKENS // TOK_DEV
    key_list = jax.random.split(jax.random.fold_in(key, 11), 6)
    counts = jax.random.randint(key_list[0], (blocks,), max(CAP // 4, 1), CAP + 1)
    full_block = jax.random.randint(key_list[1], (), 0, blocks)
    counts = jnp.where(jnp.arange(blocks) == full_block, CAP, counts)
    shuffled = jax.vmap(lambda single: jax.random.permutation(single, TOK_DEV))(jax.random.split(key_list[2], blocks))
    primary = jax.random.randint(key_list[3], (blocks, TOK_DEV), 1, EXPERTS)
    offset_id = jax.random.randint(key_list[4], (blocks, TOK_DEV), 1, EXPERTS - 1)
    secondary = 1 + (primary - 1 + offset_id) % (EXPERTS - 1)
    zero_column = jax.random.randint(key_list[5], (blocks, TOK_DEV), 0, 2)
    names_zero = shuffled < counts[:, None]
    column_one = jnp.where(names_zero, jnp.where(zero_column == 0, 0, primary), primary)
    column_two = jnp.where(names_zero, jnp.where(zero_column == 0, primary, 0), secondary)
    return jnp.stack([column_one, column_two], axis=-1).reshape(TOKENS, 2).astype(jnp.int32)


def level_of(stream_key, extent, cuts, smallest, largest):
    gain, own = 1.0, jax.random.fold_in(stream_key, 6)
    for dim, parts in cuts:
        heights = jnp.exp(jax.random.uniform(jax.random.fold_in(own, dim), (parts,), jnp.float32, smallest / len(cuts), largest / len(cuts)))
        gain = gain * jnp.repeat(heights, extent[dim] // parts).reshape([-1 if axis == dim else 1 for axis in range(len(extent))])
    return gain


def gaussian(key, dims, scale, reach, shards=(), kind=jnp.bfloat16):
    drawn = jax.random.normal(key, dims, jnp.float32) * scale
    if len(shards) > 0:
        drawn = level_of(key, dims, shards, -0.22, 0.18) * drawn
    return jnp.clip(drawn, min=-reach, max=reach).astype(kind)


def setup_inputs(seed: int = 0, part: int = 0) -> dict:
    key_of = jax.random.split(jax.random.key(seed), 13)
    part_splits = jax.random.split(jax.random.fold_in(key_of[12], part), 13)
    return {
        "hidden_in": gaussian(part_splits[0], (TOKENS, D), 1.0, 6.0, ((0, 16),)),
        "mix_norm_gain": jnp.clip(1.0 + 0.1 * jax.random.normal(key_of[1], (D,), jnp.float32), 0.5, 1.5),
        "ssm_proj": gaussian(key_of[2], (D, 2 * STATE + HEADS), D ** -0.5, 0.09375),
        "dt_bias": jnp.clip(jax.random.uniform(key_of[3], (HEADS,), jnp.float32, -1.0, 1.0), -1.0, 1.0),
        "decay_rate": jnp.clip(jnp.exp(jax.random.uniform(key_of[4], (HEADS,), jnp.float32, math.log(4.882812390860636e-06), math.log(0.05))), 4.882812390860636e-06, 0.05),
        "mixer_gain": jnp.clip(1.0 + 0.1 * jax.random.normal(key_of[5], (D,), jnp.float32), 0.5, 1.5),
        "ffn_norm_gain": jnp.clip(1.0 + 0.1 * jax.random.normal(key_of[6], (D,), jnp.float32), 0.5, 1.5),
        "router": gaussian(key_of[7], (D, EXPERTS), D ** -0.5, 0.09375),
        "routes": draw_routes(jax.random.fold_in(jax.random.fold_in(key_of[12], part), 71), part),
        "w_gate": gaussian(key_of[9], (D, FF), D ** -0.5, 0.09375, ((1, 16),)),
        "w_up": gaussian(key_of[10], (D, FF), D ** -0.5, 0.09375, ((1, 16),)),
        "w_down": gaussian(key_of[11], (FF, D), FF ** -0.5, 0.09375, ((0, 16),)),
    }


EPSILON = 1e-05
HIGHEST_MODE = lax.Precision.HIGHEST

def rms_scale(values, gain_row):
    return values * lax.rsqrt(lax.optimization_barrier(jnp.mean(values * values, axis=-1, keepdims=True)) + EPSILON) * gain_row

def span_output(span_x, span_b, span_c, span_dt, span_cum, entering, lower_mask):
    cross_dot = jnp.dot(span_c, span_b.T, precision=HIGHEST_MODE)
    log_gap = span_cum.T[:, :, None] - span_cum.T[:, None, :]
    decays = jnp.where(lower_mask[None], jnp.exp(jnp.minimum(log_gap, 0.0)), 0.0)
    weights = (cross_dot[None] * decays * span_dt.T[:, None, :]).astype(jnp.bfloat16)
    within = jnp.einsum('hts,shp->thp', weights.astype(jnp.float32), span_x.astype(jnp.float32), precision=HIGHEST_MODE)
    carried = jnp.exp(span_cum)[:, :, None] * jnp.einsum('tn,hpn->thp', span_c, entering, precision=HIGHEST_MODE)
    return within + carried

def span_state(span_x, span_b, span_dt, span_cum):
    to_end = jnp.exp(span_cum[-1][None, :] - span_cum) * span_dt
    state_weights = (to_end[:, :, None] * span_b[:, None, :]).astype(jnp.bfloat16)
    return jnp.einsum('shp,shn->hpn', span_x.astype(jnp.float32), state_weights.astype(jnp.float32), precision=HIGHEST_MODE)

def route_gates(logits, routes):
    expert_ids = jnp.arange(logits.shape[1], dtype=jnp.int32)
    chosen_logit = lax.optimization_barrier(jnp.sum(jnp.where(routes[:, :, None] == expert_ids[None, None, :], logits[:, None, :], 0.0), axis=2))
    first_zero = routes[:, 0] == 0
    routed = first_zero | (routes[:, 1] == 0)
    second_logit = jnp.where(first_zero, chosen_logit[:, 1], chosen_logit[:, 0])
    gating = jnp.where(routed, jax.nn.sigmoid(logits[:, 0] - second_logit), 0.0)
    return (gating, routed)

def reference(hidden_in, mix_norm_gain, ssm_proj, dt_bias, decay_rate, mixer_gain, ffn_norm_gain, router, routes, w_gate, w_up, w_down):
    head_size = D // HEADS
    span_count = TOKENS // SPAN
    wide_input = hidden_in.astype(jnp.float32)
    normed = rms_scale(wide_input, mix_norm_gain).astype(jnp.bfloat16)
    projected = jnp.dot(normed, ssm_proj, preferred_element_type=jnp.float32)
    b_in = projected[:, :STATE]
    c_out = projected[:, STATE:2 * STATE]
    step_size = jax.nn.softplus(projected[:, 2 * STATE:] + dt_bias)
    log_decay = -step_size * decay_rate
    lower_mask = jnp.arange(SPAN)[:, None] >= jnp.arange(SPAN)[None, :]
    lower_ones = lower_mask.astype(jnp.float32)

    def advance(carry_state, pieces):
        span_x, span_b, span_c, span_dt, span_log = pieces
        span_cum = jnp.dot(lower_ones, span_log, precision=HIGHEST_MODE)
        output = span_output(span_x, span_b, span_c, span_dt, span_cum, carry_state, lower_mask)
        updated = jnp.exp(span_cum[-1])[:, None, None] * carry_state + span_state(span_x, span_b, span_dt, span_cum)
        return (updated, output)
    pieces = (normed.reshape(span_count, SPAN, HEADS, head_size), b_in.reshape(span_count, SPAN, STATE), c_out.reshape(span_count, SPAN, STATE), step_size.reshape(span_count, SPAN, HEADS), log_decay.reshape(span_count, SPAN, HEADS))
    final_state, ssm_out = lax.scan(advance, jnp.zeros((HEADS, head_size, STATE), jnp.float32), pieces)
    ssm_out = ssm_out.reshape(TOKENS, HEADS, head_size)
    scaled = ssm_out * lax.rsqrt(lax.optimization_barrier(jnp.mean(ssm_out * ssm_out, axis=-1, keepdims=True)) + EPSILON) * mixer_gain.reshape(HEADS, head_size)
    after_mixer = (wide_input + scaled.reshape(TOKENS, D)).astype(jnp.bfloat16)
    ffn_in = rms_scale(after_mixer.astype(jnp.float32), ffn_norm_gain).astype(jnp.bfloat16)
    logits = jnp.dot(ffn_in, router, preferred_element_type=jnp.float32)
    gating, routed = route_gates(logits, routes)
    blocks = TOKENS // TOK_DEV
    routed_blocks = routed.reshape(blocks, TOK_DEV)
    slot_rank = jnp.cumsum(routed_blocks.astype(jnp.int32), axis=1).astype(jnp.int32) - 1
    slot_ids = jnp.arange(CAP, dtype=jnp.int32)
    select_map = routed_blocks[:, None, :] & (slot_rank[:, None, :] == slot_ids[None, :, None])
    ffn_blocks = ffn_in.reshape(blocks, TOK_DEV, D)

    def select_rows(inputs_pair):
        return jnp.dot(inputs_pair[0].astype(jnp.bfloat16), inputs_pair[1], preferred_element_type=jnp.float32).astype(jnp.bfloat16)
    expert_in = lax.map(select_rows, (select_map, ffn_blocks)).reshape(blocks * CAP, D)
    gate_part = jnp.dot(expert_in, w_gate, preferred_element_type=jnp.float32)
    up_part = jnp.dot(expert_in, w_up, preferred_element_type=jnp.float32)
    hidden = (jax.nn.silu(gate_part) * up_part).astype(jnp.bfloat16)
    expert_out = jnp.dot(hidden, w_down, preferred_element_type=jnp.float32).reshape(blocks, CAP, D)
    returned = jnp.einsum('bct,bcd->btd', select_map.astype(jnp.float32), expert_out, precision=HIGHEST_MODE).reshape(TOKENS, D)
    return (after_mixer.astype(jnp.float32) + gating[:, None] * returned).astype(jnp.bfloat16)
```

```python
import functools

import jax
import jax.numpy as jnp
from jax import lax
from jax.experimental import pallas as pl
from jax.experimental.pallas import tpu as pltpu
from jax.sharding import PartitionSpec as P

CAP = 16
EPS = 1e-05
HI = lax.Precision.HIGHEST
MESH = pl.DeviceIdType.MESH
F32 = jnp.float32
BF16 = jnp.bfloat16


def remote(src, dst, send, recv, target):
    return pltpu.make_async_remote_copy(
        src_ref=src,
        dst_ref=dst,
        send_sem=send,
        recv_sem=recv,
        device_id={"seq": target},
        device_id_type=MESH,
    )


def iota(shape, dim):
    return lax.broadcasted_iota(jnp.int32, shape, dim)


def block_kernel(
    n,
    hid,
    gain,
    proj,
    bias,
    rate,
    mgain,
    fgain,
    router,
    routes,
    wg_hbm,
    wu_hbm,
    wd_hbm,
    am_out,
    own_out,
    sel_out,
    gate_out,
    wg,
    wu,
    wd,
    xn,
    within,
    am,
    acc,
    cum3,
    cumt,
    dtt,
    tet,
    bt,
    crossm,
    phi,
    plo,
    msg,
    inbox,
    scan_out,
    ent,
    gath,
    part,
    prt,
    rbuf,
    w_sem,
    am_sem,
    a_send,
    a_recv,
    b_send,
    b_recv,
    g_send,
    g_recv,
    d_send,
    d_recv,
    p_send,
    p_recv,
    r_send,
    r_recv,
):
    tok, width = hid.shape
    heads = bias.shape[0]
    lanes = width // heads
    state = (proj.shape[1] - heads) // 2
    owners = msg.shape[0]
    per = heads // owners
    chips = n // 2
    half_ring = chips // 2
    hw = width // 2
    me = lax.axis_index("seq")
    core = me % 2
    chip = me // 2
    odd = chip % 2
    pos = (1 - odd) * (chip // 2) + odd * (chips - 1 - chip // 2)

    def device_at(place):
        place = (place + 2 * chips) % chips
        high = place // half_ring
        held = (1 - high) * (2 * place) + high * (2 * (chips - 1 - place) + 1)
        return held * 2 + core

    def slot_at(place, which):
        return which * chips + (place + 2 * chips) % chips

    partner = me + 1 - 2 * core

    barrier = pltpu.get_barrier_semaphore()
    for d in range(1, n):
        pl.semaphore_signal(
            barrier, inc=1, device_id={"seq": (me + d) % n}, device_id_type=MESH
        )

    loads = [
        pltpu.make_async_copy(a, b, w_sem.at[k])
        for k, (a, b) in enumerate(((wg_hbm, wg), (wu_hbm, wu), (wd_hbm, wd)))
    ]
    for load in loads:
        load.start()

    def norm_rows(i, _):
        rows = pl.ds(pl.multiple_of(i * 16, 16), 16)
        x = hid[rows, :].astype(F32)
        ms = jnp.mean(x * x, axis=-1, keepdims=True)
        xn[rows, :] = (x * lax.rsqrt(ms + EPS) * gain[...]).astype(BF16)
        return 0

    lax.fori_loop(0, tok // 16, norm_rows, 0)

    p = jnp.dot(xn[...], proj[...], preferred_element_type=F32)
    p_hi = p.astype(BF16)
    phi[...] = p_hi
    plo[...] = (p - p_hi.astype(F32)).astype(BF16)
    pt = p.T
    b_t = pt[0:state]
    v = pt[2 * state :] + bias[...]
    dt = jnp.maximum(v, 0.0) + jnp.log(1.0 + jnp.exp(-jnp.abs(v)))
    upper = (iota((tok, tok), 0) <= iota((tok, tok), 1)).astype(F32)
    c_t = jnp.dot(-dt * rate[...], upper, precision=HI, preferred_element_type=F32)
    bt[...] = b_t
    dtt[...] = dt
    cumt[...] = c_t
    tet[...] = jnp.exp(c_t[:, tok - 1 : tok] - c_t) * dt
    c1 = c_t.astype(BF16).astype(F32)
    c2 = (c_t - c1).astype(BF16).astype(F32)
    c3 = c_t - c1 - c2
    pad = jnp.zeros((128 - 3 * heads, tok), F32)
    cum3[...] = jnp.concatenate([c1, c2, c3, pad], axis=0).T.astype(BF16)

    def spread(h):
        row = iota((128, lanes), 0)
        pick = ((row % heads) == h) & (row < 3 * heads)
        return jnp.where(pick, 1.0, 0.0).astype(BF16)

    def state_head(h, _):
        cols = pl.ds(pl.multiple_of(h * lanes, lanes), lanes)
        inner = pl.ds(pl.multiple_of((h % per) * lanes, lanes), lanes)
        sw = (bt[...] * tet[pl.ds(h, 1), :]).astype(BF16)
        s = jnp.dot(sw, xn[:, cols], preferred_element_type=F32)
        msg[h // per, 0:state, inner] = s.astype(BF16)
        last = jnp.dot(cum3[tok - 16 : tok, :], spread(h), preferred_element_type=F32)
        d = jnp.exp(last[15:16, :])
        d_hi = d.astype(BF16).astype(F32)
        row = iota((16, lanes), 0)
        packed = jnp.where(row == 0, d_hi, jnp.where(row == 1, d - d_hi, 0.0))
        msg[h // per, state : state + 16, inner] = packed.astype(BF16)
        return 0

    lax.fori_loop(0, heads, state_head, 0)

    pl.semaphore_wait(barrier, n - 1)

    def to_owner(owner, source):
        return remote(
            msg.at[owner], inbox.at[source], a_send.at[owner], a_recv.at[source], owner
        )

    def to_reader(reader, source):
        return remote(
            scan_out.at[reader],
            ent.at[source],
            b_send.at[reader],
            b_recv.at[source],
            reader,
        )

    every = owners == n

    def for_owner(index, run):
        if every:
            run()
        else:
            pl.when(index < owners)(run)

    for d in range(1, n):
        dest = (me + d) % n
        for_owner(dest, lambda: to_owner(dest, me).start())

    z = jnp.concatenate(
        [
            jnp.zeros((state, tok), F32),
            bt[...],
            jnp.zeros((p.shape[1] - 2 * state, tok), F32),
        ],
        axis=0,
    )
    cross = jnp.dot(p, z, precision=HI, preferred_element_type=F32)
    crossm[...] = jnp.where(iota((tok, tok), 0) >= iota((tok, tok), 1), cross, 0.0)

    mid = tok // 2

    def within_head(h, _):
        cols = pl.ds(pl.multiple_of(h * lanes, lanes), lanes)
        ch = jnp.dot(cum3[...], spread(h), preferred_element_type=F32)
        crow = cumt[pl.ds(h, 1), :]
        drow = dtt[pl.ds(h, 1), :]
        for k in range(2):
            rows = slice(k * mid, (k + 1) * mid)
            total = None
            for j in range(k + 1):
                over = slice(j * mid, (j + 1) * mid)
                gap = ch[rows, :] - crow[:, over]
                w = crossm[rows, over] * jnp.exp(jnp.minimum(gap, 0.0)) * drow[:, over]
                term = jnp.dot(
                    w.astype(BF16), xn[over, cols], preferred_element_type=F32
                )
                total = term if total is None else total + term
            within[rows, cols] = total
        return 0

    lax.fori_loop(0, heads // 2, within_head, 0)

    def scan_all():
        inbox[me] = msg[me]
        for d in range(1, n):
            to_owner(0, (me + d) % n).wait_recv()
        running = jnp.zeros((state, per * lanes), F32)
        for j in range(n):
            scan_out[j] = running.astype(BF16)
            decay = (
                inbox[j, state : state + 1, :].astype(F32)
                + inbox[j, state + 1 : state + 2, :].astype(F32)
            )
            running = decay * running + inbox[j, 0:state, :].astype(F32)
        ent[me] = scan_out[me]
        for d in range(1, n):
            dest = (me + d) % n
            to_reader(dest, me).start()

    for_owner(me, scan_all)

    lax.fori_loop(heads // 2, heads, within_head, 0)

    for d in range(1, n):
        source = (me + d) % n
        for_owner(source, lambda: to_reader(0, source).wait_recv())

    acc[...] = jnp.zeros_like(acc)

    def mix_head(h, _):
        cols = pl.ds(pl.multiple_of(h * lanes, lanes), lanes)
        inner = pl.ds(pl.multiple_of((h % per) * lanes, lanes), lanes)
        e = ent[h // per, :, inner]
        zero = jnp.zeros((state, lanes), BF16)
        rest = jnp.zeros((phi.shape[1] - 2 * state, lanes), BF16)
        ez = jnp.concatenate([zero, e, rest], axis=0)
        carried = jnp.dot(phi[...], ez, preferred_element_type=F32) + jnp.dot(
            plo[...], ez, preferred_element_type=F32
        )
        ch = jnp.dot(cum3[...], spread(h), preferred_element_type=F32)
        o = within[:, cols] + jnp.exp(ch) * carried
        ms = jnp.mean(o * o, axis=-1, keepdims=True)
        y = hid[:, cols].astype(F32) + o * lax.rsqrt(ms + EPS) * mgain[:, cols]
        y = y.astype(BF16)
        am[:, cols] = y
        yf = y.astype(F32)
        acc[...] += yf * yf
        return 0

    lax.fori_loop(0, heads, mix_head, 0)

    am_copy = pltpu.make_async_copy(am, am_out, am_sem)
    am_copy.start()

    total = jnp.sum(acc[...], axis=-1, keepdims=True)
    acc[...] = jnp.broadcast_to(lax.rsqrt(total / width + EPS), acc.shape)

    def ffn_rows(i, _):
        rows = pl.ds(pl.multiple_of(i * 16, 16), 16)
        x = am[rows, :].astype(F32)
        xn[rows, :] = (x * acc[rows, 0:1] * fgain[...]).astype(BF16)
        return 0

    lax.fori_loop(0, tok // 16, ffn_rows, 0)

    r0 = routes[:, 0:1]
    r1 = routes[:, 1:2]
    hit = jnp.where((r0 == 0) | (r1 == 0), 1.0, 0.0)
    lower = (iota((tok, tok), 0) >= iota((tok, tok), 1)).astype(BF16)
    wide = jnp.broadcast_to(hit, (tok, 128))
    rank = jnp.dot(lower, wide.astype(BF16), preferred_element_type=F32)
    lane = iota((tok, 128), 1)
    place = (rank - 1.0).astype(jnp.int32)
    sel_t = jnp.where(((lane % CAP) == place) & (lane < 2 * CAP), wide, 0.0)
    sel = sel_t.T[0:CAP].astype(BF16)
    sel_out[...] = sel_t.astype(BF16)
    mine = slot_at(pos, core)
    gath[mine] = jnp.dot(sel, xn[...], preferred_element_type=F32).astype(BF16)

    def cut(h):
        return pl.ds(h * hw, hw)

    def ring(way, s, h, place):
        step = 1 - 2 * way
        block = gath.at[slot_at(place, core), :, cut(h)]
        return remote(
            block,
            block,
            g_send.at[way, s, h],
            g_recv.at[way, s, h],
            device_at(pos + step),
        )

    def across(way, s, h, place, which):
        block = gath.at[slot_at(place, which), :, cut(h)]
        return remote(
            block, block, d_send.at[way, s, h], d_recv.at[way, s, h], partner
        )

    started = []

    def go(copy):
        copy.start()
        started.append(copy)

    def used(way, s, h):
        return s < half_ring - 1 or h == way

    for h in range(2):
        for way in range(2):
            hh = h if way == 0 else 1 - h
            if used(way, 0, hh):
                go(ring(way, 0, hh, pos))
    def own_across(h, slot):
        block = gath.at[slot, :, cut(h)]
        return remote(
            block,
            block,
            d_send.at[h, half_ring, 0],
            d_recv.at[h, half_ring, 0],
            partner,
        )

    for h in range(2):
        go(own_across(h, mine))

    logits = jnp.dot(xn[...], router[...], preferred_element_type=F32)
    other = jnp.where(r0 == 0, r1, r0)
    picked = jnp.sum(
        jnp.where(iota(logits.shape, 1) == other, logits, 0.0), axis=1, keepdims=True
    )
    gate = jnp.where(hit > 0.0, 1.0 / (1.0 + jnp.exp(picked - logits[:, 0:1])), 0.0)
    gate_out[...] = jnp.broadcast_to(gate, gate_out.shape)

    for s in range(half_ring):
        for h in range(2):
            for way in range(2):
                hh = h if way == 0 else 1 - h
                if not used(way, s, hh):
                    continue
                step = 1 - 2 * way
                place = pos - step * (1 + s)
                ring(way, s, hh, place).wait_recv()
                if s + 1 < half_ring and used(way, s + 1, hh):
                    go(ring(way, s + 1, hh, place))
                go(across(way, s, hh, place, core))
    for h in range(2):
        own_across(h, slot_at(pos, 1 - core)).wait_recv()
    for s in range(half_ring):
        for way in range(2):
            for h in range(2):
                if used(way, s, h):
                    step = 1 - 2 * way
                    across(way, s, h, pos - step * (1 + s), 1 - core).wait_recv()

    for load in loads:
        load.wait()
    rows_all = n * CAP
    x_all = gath[...].reshape(rows_all, width)
    g = jnp.dot(x_all, wg[...], preferred_element_type=F32)
    u = jnp.dot(x_all, wu[...], preferred_element_type=F32)
    hidden = (g / (1.0 + jnp.exp(-g)) * u).astype(BF16)
    step_w = 512
    for k in range(width // step_w):
        c = slice(k * step_w, (k + 1) * step_w)
        part[:, :, c] = (
            jnp.dot(hidden, wd[:, c], preferred_element_type=F32)
            .astype(BF16)
            .reshape(n, CAP, step_w)
        )
    swap = remote(
        part.at[pl.ds((1 - core) * chips, chips)], prt, p_send, p_recv, partner
    )
    go(swap)
    swap.wait_recv()

    def pair_sum(i, _):
        at = core * chips + i
        part[at] = (part[at].astype(F32) + prt[i].astype(F32)).astype(BF16)
        return 0

    lax.fori_loop(0, chips, pair_sum, 0)

    def reduce_copy(way, s, h):
        step = 1 - 2 * way
        place = pos + step * (half_ring - s)
        return remote(
            part.at[slot_at(place, core), :, cut(h)],
            rbuf.at[way, s, h],
            r_send.at[way, s, h],
            r_recv.at[way, s, h],
            device_at(pos + step),
        )

    def carries(way, s, h):
        return s > 0 or h == way

    for s in range(half_ring):
        for h in range(2):
            for way in range(2):
                hh = h if way == 0 else 1 - h
                if not carries(way, s, hh):
                    continue
                if s > 0 and carries(way, s - 1, hh):
                    reduce_copy(way, s - 1, hh).wait_recv()
                    step = 1 - 2 * way
                    at = slot_at(pos + step * (half_ring - s), core)
                    cc = slice(hh * hw, (hh + 1) * hw)
                    part[at, :, cc] = (
                        part[at, :, cc].astype(F32)
                        + rbuf[way, s - 1, hh].astype(F32)
                    ).astype(BF16)
                go(reduce_copy(way, s, hh))
    for h in range(2):
        cc = slice(h * hw, (h + 1) * hw)
        own = part[mine, :, cc].astype(F32)
        for way in range(2):
            if carries(way, half_ring - 1, h):
                reduce_copy(way, half_ring - 1, h).wait_recv()
                own += rbuf[way, half_ring - 1, h].astype(F32)
        own_hi = own.astype(BF16)
        own_out[0:CAP, cc] = own_hi
        own_out[CAP : 2 * CAP, cc] = (own - own_hi.astype(F32)).astype(BF16)

    am_copy.wait()
    for copy in started:
        copy.wait_send()
    for d in range(1, n):
        dest = (me + d) % n
        for_owner(dest, lambda: to_owner(dest, me).wait_send())

    def drain():
        for d in range(1, n):
            to_reader((me + d) % n, me).wait_send()

    for_owner(me, drain)


def combine_kernel(am, sel, gate, own, out):
    back = jnp.dot(sel[:, 0 : own.shape[0]], own[...], preferred_element_type=F32)
    out[...] = (am[...].astype(F32) + gate[:, 0:1] * back).astype(BF16)


def solution(mesh):
    n = mesh.shape["seq"]

    def body(
        hid, gain, proj, bias, rate, mgain, fgain, router, routes, wg, wu, wd
    ):
        tok, width = hid.shape
        heads = bias.shape[0]
        lanes = width // heads
        cols = proj.shape[1]
        state = (cols - heads) // 2
        owners = min(n, heads)
        per = heads // owners
        chips = n // 2
        half_ring = chips // 2
        vm = pl.BlockSpec(memory_space=pltpu.VMEM)
        anyspec = pl.BlockSpec(memory_space=pl.ANY)
        dma = pltpu.SemaphoreType.DMA
        am, own, sel, gate = pl.pallas_call(
            functools.partial(block_kernel, n),
            out_shape=[
                jax.ShapeDtypeStruct((tok, width), BF16),
                jax.ShapeDtypeStruct((2 * CAP, width), BF16),
                jax.ShapeDtypeStruct((tok, 128), BF16),
                jax.ShapeDtypeStruct((tok, 128), F32),
            ],
            in_specs=[vm] * 9 + [anyspec] * 3,
            out_specs=[anyspec, vm, vm, vm],
            scratch_shapes=[
                pltpu.VMEM(wg.shape, BF16),
                pltpu.VMEM(wu.shape, BF16),
                pltpu.VMEM(wd.shape, BF16),
                pltpu.VMEM((tok, width), BF16),
                pltpu.VMEM((tok, width), F32),
                pltpu.VMEM((tok, width), BF16),
                pltpu.VMEM((tok, 128), F32),
                pltpu.VMEM((tok, 128), BF16),
                pltpu.VMEM((heads, tok), F32),
                pltpu.VMEM((heads, tok), F32),
                pltpu.VMEM((heads, tok), F32),
                pltpu.VMEM((state, tok), F32),
                pltpu.VMEM((tok, tok), F32),
                pltpu.VMEM((tok, cols), BF16),
                pltpu.VMEM((tok, cols), BF16),
                pltpu.VMEM((owners, state + 16, per * lanes), BF16),
                pltpu.VMEM((n, state + 16, per * lanes), BF16),
                pltpu.VMEM((n, state, per * lanes), BF16),
                pltpu.VMEM((owners, state, per * lanes), BF16),
                pltpu.VMEM((n, CAP, width), BF16),
                pltpu.VMEM((n, CAP, width), BF16),
                pltpu.VMEM((chips, CAP, width), BF16),
                pltpu.VMEM((2, half_ring, 2, CAP, width // 2), BF16),
                dma((3,)),
                dma,
                dma((n,)),
                dma((n,)),
                dma((n,)),
                dma((n,)),
                dma((2, half_ring, 2)),
                dma((2, half_ring, 2)),
                dma((2, half_ring + 1, 2)),
                dma((2, half_ring + 1, 2)),
                dma,
                dma,
                dma((2, half_ring, 2)),
                dma((2, half_ring, 2)),
            ],
            compiler_params=pltpu.CompilerParams(
                collective_id=0,
                has_side_effects=True,
                vmem_limit_bytes=60 * 1024 * 1024,
            ),
        )(
            hid,
            gain.reshape(1, width),
            proj,
            bias.reshape(heads, 1),
            rate.reshape(heads, 1),
            mgain.reshape(1, width),
            fgain.reshape(1, width),
            router,
            routes,
            wg,
            wu,
            wd,
        )
        block = width // 4
        return pl.pallas_call(
            combine_kernel,
            grid=(4,),
            out_shape=jax.ShapeDtypeStruct((tok, width), BF16),
            in_specs=[
                pl.BlockSpec((tok, block), lambda i: (0, i)),
                pl.BlockSpec((tok, 128), lambda i: (0, 0)),
                pl.BlockSpec((tok, 128), lambda i: (0, 0)),
                pl.BlockSpec((2 * CAP, block), lambda i: (0, i)),
            ],
            out_specs=pl.BlockSpec((tok, block), lambda i: (0, i)),
        )(am, sel, gate, own)

    both = P(("docs", "seq"), None)
    in_specs = (
        both, P(), P(), P(), P(), P(), P(), P(), both,
        P(None, "seq"), P(None, "seq"), P("seq", None),
    )
    return jax.shard_map(
        body, mesh=mesh, in_specs=in_specs, out_specs=both, check_vma=False
    )
```

```python
import functools

import jax
import jax.numpy as jnp
from jax import lax
from jax.experimental import pallas as pl
from jax.experimental.pallas import tpu as pltpu
from jax.sharding import PartitionSpec as P

CAP = 16
EPS = 1e-05
HI = lax.Precision.HIGHEST
MESH = pl.DeviceIdType.MESH
F32 = jnp.float32
BF16 = jnp.bfloat16


def remote(src, dst, send, recv, target):
    return pltpu.make_async_remote_copy(
        src_ref=src,
        dst_ref=dst,
        send_sem=send,
        recv_sem=recv,
        device_id={"seq": target},
        device_id_type=MESH,
    )


def across_last(a, b):
    return lax.dot_general(a, b, (((1,), (1,)), ((), ())), preferred_element_type=F32)


def iota(shape, dim):
    return lax.broadcasted_iota(jnp.int32, shape, dim)


def block_kernel(
    n,
    hid,
    gain,
    proj,
    bias,
    rate,
    mgain,
    fgain,
    router,
    routes,
    wg_hbm,
    wu_hbm,
    wd_hbm,
    am_out,
    own_out,
    sel_out,
    wg,
    wu,
    wd,
    xn,
    within,
    am,
    wsel,
    hsel,
    ysel,
    cum3,
    cumt,
    dtt,
    tet,
    bt,
    crossm,
    phi,
    plo,
    msg,
    inbox,
    scan_out,
    ent,
    gath,
    part,
    prt,
    rbuf,
    w_sem,
    am_sem,
    a_send,
    a_recv,
    b_send,
    b_recv,
    g_send,
    g_recv,
    d_send,
    d_recv,
    p_send,
    p_recv,
    r_send,
    r_recv,
):
    tok, width = hid.shape
    heads = bias.shape[1]
    lanes = width // heads
    state = (proj.shape[0] - heads) // 2
    owners = msg.shape[0]
    per = heads // owners
    chips = n // 2
    half_ring = chips // 2
    hw = width // 2
    me = lax.axis_index("seq")
    core = me % 2
    chip = me // 2
    odd = chip % 2
    pos = (1 - odd) * (chip // 2) + odd * (chips - 1 - chip // 2)

    def device_at(place):
        place = (place + 2 * chips) % chips
        high = place // half_ring
        held = (1 - high) * (2 * place) + high * (2 * (chips - 1 - place) + 1)
        return held * 2 + core

    def slot_at(place, which):
        return which * chips + (place + 2 * chips) % chips

    partner = me + 1 - 2 * core

    barrier = pltpu.get_barrier_semaphore()
    for d in range(1, n):
        pl.semaphore_signal(
            barrier, inc=1, device_id={"seq": (me + d) % n}, device_id_type=MESH
        )

    loads = [
        pltpu.make_async_copy(a, b, w_sem.at[k])
        for k, (a, b) in enumerate(((wg_hbm, wg), (wu_hbm, wu), (wd_hbm, wd)))
    ]
    for load in loads:
        load.start()

    def norm_rows(i, _):
        rows = pl.ds(pl.multiple_of(i * 16, 16), 16)
        x = hid[rows, :].astype(F32)
        ms = jnp.mean(x * x, axis=-1, keepdims=True)
        xn[rows, :] = (x * lax.rsqrt(ms + EPS) * gain[...]).astype(BF16)
        return 0

    lax.fori_loop(0, tok // 16, norm_rows, 0)

    p = across_last(xn[...], proj[...])
    p_hi = p.astype(BF16)
    phi[...] = p_hi
    plo[...] = (p - p_hi.astype(F32)).astype(BF16)
    pt = p.T
    b_t = pt[0:state]
    eye = iota((heads, heads), 0) == iota((heads, heads), 1)
    bias_col = jnp.sum(jnp.where(eye, bias[...], 0.0), axis=1, keepdims=True)
    rate_col = jnp.sum(jnp.where(eye, rate[...], 0.0), axis=1, keepdims=True)
    v = pt[2 * state :] + bias_col
    dt = jnp.maximum(v, 0.0) + jnp.log(1.0 + jnp.exp(-jnp.abs(v)))
    upper = (iota((tok, tok), 0) <= iota((tok, tok), 1)).astype(F32)
    c_t = jnp.dot(-dt * rate_col, upper, precision=HI, preferred_element_type=F32)
    bt[...] = b_t
    dtt[...] = dt
    cumt[...] = c_t
    tet[...] = jnp.exp(c_t[:, tok - 1 : tok] - c_t) * dt
    c1 = c_t.astype(BF16).astype(F32)
    c2 = (c_t - c1).astype(BF16).astype(F32)
    c3 = c_t - c1 - c2
    pad = jnp.zeros((128 - 3 * heads, tok), F32)
    cum3[...] = jnp.concatenate([c1, c2, c3, pad], axis=0).T.astype(BF16)

    def spread(h):
        row = iota((128, lanes), 0)
        pick = ((row % heads) == h) & (row < 3 * heads)
        return jnp.where(pick, 1.0, 0.0).astype(BF16)

    def state_head(h, _):
        cols = pl.ds(pl.multiple_of(h * lanes, lanes), lanes)
        inner = pl.ds(pl.multiple_of((h % per) * lanes, lanes), lanes)
        sw = (bt[...] * tet[pl.ds(h, 1), :]).astype(BF16)
        s = jnp.dot(sw, xn[:, cols], preferred_element_type=F32)
        msg[h // per, 0:state, inner] = s.astype(BF16)
        last = jnp.dot(cum3[tok - 16 : tok, :], spread(h), preferred_element_type=F32)
        d = jnp.exp(last[15:16, :])
        d_hi = d.astype(BF16).astype(F32)
        row = iota((16, lanes), 0)
        packed = jnp.where(row == 0, d_hi, jnp.where(row == 1, d - d_hi, 0.0))
        msg[h // per, state : state + 16, inner] = packed.astype(BF16)
        return 0

    lax.fori_loop(0, heads, state_head, 0)

    pl.semaphore_wait(barrier, n - 1)

    def to_owner(owner, source):
        return remote(
            msg.at[owner], inbox.at[source], a_send.at[owner], a_recv.at[source], owner
        )

    def to_reader(reader, source):
        return remote(
            scan_out.at[reader],
            ent.at[source],
            b_send.at[reader],
            b_recv.at[source],
            reader,
        )

    every = owners == n

    def for_owner(index, run):
        if every:
            run()
        else:
            pl.when(index < owners)(run)

    for d in range(1, n):
        dest = (me + d) % n
        for_owner(dest, lambda: to_owner(dest, me).start())

    z = jnp.concatenate(
        [
            jnp.zeros((state, tok), F32),
            bt[...],
            jnp.zeros((p.shape[1] - 2 * state, tok), F32),
        ],
        axis=0,
    )
    cross = jnp.dot(p, z, precision=HI, preferred_element_type=F32)
    crossm[...] = jnp.where(iota((tok, tok), 0) >= iota((tok, tok), 1), cross, 0.0)

    r0 = routes[0:1, :]
    r1 = routes[1:2, :]
    hit = jnp.where((r0 == 0) | (r1 == 0), 1.0, 0.0)
    other = jnp.where(r0 == 0, r1, r0).astype(F32)
    wide = jnp.broadcast_to(hit, (CAP, tok))
    rank = jnp.dot(
        wide.astype(BF16), upper.astype(BF16), preferred_element_type=F32
    )
    sel_f = jnp.where((rank - 1.0).astype(jnp.int32) == iota((CAP, tok), 0), wide, 0.0)
    other_sel = jnp.sum(sel_f * other, axis=1, keepdims=True)
    sel = sel_f.astype(BF16)
    blank = jnp.zeros((128 - 2 * CAP, tok), F32)
    sel_out[...] = jnp.concatenate([sel_f, sel_f, blank], axis=0).T.astype(BF16)

    def pick(value):
        return jnp.dot(sel, value, preferred_element_type=F32).astype(BF16)

    hsel[...] = pick(hid[...])
    phi_sel = pick(phi[...])
    plo_sel = pick(plo[...])
    cum_sel = pick(cum3[...])

    mid = tok // 2

    def within_head(h, _):
        cols = pl.ds(pl.multiple_of(h * lanes, lanes), lanes)
        ch = jnp.dot(cum3[...], spread(h), preferred_element_type=F32)
        crow = cumt[pl.ds(h, 1), :]
        drow = dtt[pl.ds(h, 1), :]
        chosen = None
        for k in range(2):
            rows = slice(k * mid, (k + 1) * mid)
            total = None
            for j in range(k + 1):
                over = slice(j * mid, (j + 1) * mid)
                gap = ch[rows, :] - crow[:, over]
                w = crossm[rows, over] * jnp.exp(jnp.minimum(gap, 0.0)) * drow[:, over]
                term = jnp.dot(
                    w.astype(BF16), xn[over, cols], preferred_element_type=F32
                )
                total = term if total is None else total + term
            within[rows, cols] = total
            top = total.astype(BF16)
            low = (total - top.astype(F32)).astype(BF16)
            got = jnp.dot(
                sel[:, rows], top, preferred_element_type=F32
            ) + jnp.dot(sel[:, rows], low, preferred_element_type=F32)
            chosen = got if chosen is None else chosen + got
        wsel[:, cols] = chosen
        return 0

    lax.fori_loop(0, heads // 2, within_head, 0)

    def scan_all():
        inbox[me] = msg[me]
        for d in range(1, n):
            to_owner(0, (me + d) % n).wait_recv()
        running = jnp.zeros((state, per * lanes), F32)
        for j in range(n):
            scan_out[j] = running.astype(BF16)
            decay = (
                inbox[j, state : state + 1, :].astype(F32)
                + inbox[j, state + 1 : state + 2, :].astype(F32)
            )
            running = decay * running + inbox[j, 0:state, :].astype(F32)
        ent[me] = scan_out[me]
        for d in range(1, n):
            dest = (me + d) % n
            to_reader(dest, me).start()

    for_owner(me, scan_all)

    lax.fori_loop(heads // 2, heads, within_head, 0)

    for d in range(1, n):
        source = (me + d) % n
        for_owner(source, lambda: to_reader(0, source).wait_recv())

    def mixed(h, c_hi, c_lo, cum, inside, base):
        cols = pl.ds(pl.multiple_of(h * lanes, lanes), lanes)
        inner = pl.ds(pl.multiple_of((h % per) * lanes, lanes), lanes)
        e = ent[h // per, :, inner]
        zero = jnp.zeros((state, lanes), BF16)
        rest = jnp.zeros((phi.shape[1] - 2 * state, lanes), BF16)
        ez = jnp.concatenate([zero, e, rest], axis=0)
        carried = jnp.dot(c_hi, ez, preferred_element_type=F32) + jnp.dot(
            c_lo, ez, preferred_element_type=F32
        )
        ch = jnp.dot(cum, spread(h), preferred_element_type=F32)
        o = inside[:, cols] + jnp.exp(ch) * carried
        ms = jnp.mean(o * o, axis=-1, keepdims=True)
        y = base[:, cols].astype(F32) + o * lax.rsqrt(ms + EPS) * mgain[:, cols]
        return y.astype(BF16)

    def mix_chosen(i, _):
        for k in range(4):
            h = i * 4 + k
            cols = pl.ds(pl.multiple_of(h * lanes, lanes), lanes)
            ysel[:, cols] = mixed(h, phi_sel, plo_sel, cum_sel, wsel, hsel)
        return 0

    lax.fori_loop(0, heads // 4, mix_chosen, 0)

    x = ysel[...].astype(F32)
    ms = jnp.mean(x * x, axis=-1, keepdims=True)
    chosen_in = (x * lax.rsqrt(ms + EPS) * fgain[...]).astype(BF16)
    mine = slot_at(pos, core)
    gath[mine] = chosen_in

    def mix_head(h, _):
        cols = pl.ds(pl.multiple_of(h * lanes, lanes), lanes)
        am[:, cols] = mixed(h, phi[...], plo[...], cum3[...], within, hid)
        return 0

    def cut(h):
        return pl.ds(h * hw, hw)

    def ring(way, s, h, place):
        step = 1 - 2 * way
        block = gath.at[slot_at(place, core), :, cut(h)]
        return remote(
            block,
            block,
            g_send.at[way, s, h],
            g_recv.at[way, s, h],
            device_at(pos + step),
        )

    def across(way, s, h, place, which):
        block = gath.at[slot_at(place, which), :, cut(h)]
        return remote(
            block, block, d_send.at[way, s, h], d_recv.at[way, s, h], partner
        )

    started = []

    def go(copy):
        copy.start()
        started.append(copy)

    def used(way, s, h):
        return s < half_ring - 1 or h == way

    for h in range(2):
        for way in range(2):
            hh = h if way == 0 else 1 - h
            if used(way, 0, hh):
                go(ring(way, 0, hh, pos))
    def own_across(h, slot):
        block = gath.at[slot, :, cut(h)]
        return remote(
            block,
            block,
            d_send.at[h, half_ring, 0],
            d_recv.at[h, half_ring, 0],
            partner,
        )

    for h in range(2):
        go(own_across(h, mine))

    logits = across_last(chosen_in, router[...])
    picked = jnp.sum(
        jnp.where(iota(logits.shape, 1) == other_sel.astype(jnp.int32), logits, 0.0),
        axis=1,
        keepdims=True,
    )
    gate = 1.0 / (1.0 + jnp.exp(picked - logits[:, 0:1]))

    pieces = 2 * half_ring
    done = 0

    for s in range(half_ring):
        for h in range(2):
            for way in range(2):
                hh = h if way == 0 else 1 - h
                if not used(way, s, hh):
                    continue
                step = 1 - 2 * way
                place = pos - step * (1 + s)
                ring(way, s, hh, place).wait_recv()
                if s + 1 < half_ring and used(way, s + 1, hh):
                    go(ring(way, s + 1, hh, place))
                go(across(way, s, hh, place, core))
            upto = (2 * s + h + 1) * heads // pieces
            lax.fori_loop(done, upto, mix_head, 0)
            done = upto
    am_copy = pltpu.make_async_copy(am, am_out, am_sem)
    am_copy.start()
    for h in range(2):
        own_across(h, slot_at(pos, 1 - core)).wait_recv()
    for s in range(half_ring):
        for way in range(2):
            for h in range(2):
                if used(way, s, h):
                    step = 1 - 2 * way
                    across(way, s, h, pos - step * (1 + s), 1 - core).wait_recv()

    for load in loads:
        load.wait()
    rows_all = n * CAP
    x_all = gath[...].reshape(rows_all, width)
    g = across_last(x_all, wg[...])
    u = across_last(x_all, wu[...])
    hidden = (g / (1.0 + jnp.exp(-g)) * u).astype(BF16)
    step_w = hw // 4

    def swap(h):
        return remote(
            part.at[pl.ds((1 - core) * chips, chips), :, cut(h)],
            prt.at[:, :, cut(h)],
            p_send.at[h],
            p_recv.at[h],
            partner,
        )

    for h in range(2):
        for k in range(4):
            c = slice(h * hw + k * step_w, h * hw + (k + 1) * step_w)
            part[:, :, c] = (
                jnp.dot(hidden, wd[:, c], preferred_element_type=F32)
                .astype(BF16)
                .reshape(n, CAP, step_w)
            )
        go(swap(h))

    def pair_sum(h):
        swap(h).wait_recv()
        cc = slice(h * hw, (h + 1) * hw)

        def one(i, _):
            at = core * chips + i
            part[at, :, cc] = (
                part[at, :, cc].astype(F32) + prt[i, :, cc].astype(F32)
            ).astype(BF16)
            return 0

        lax.fori_loop(0, chips, one, 0)

    def reduce_copy(way, s, h):
        step = 1 - 2 * way
        place = pos + step * (half_ring - s)
        return remote(
            part.at[slot_at(place, core), :, cut(h)],
            rbuf.at[way, s, h],
            r_send.at[way, s, h],
            r_recv.at[way, s, h],
            device_at(pos + step),
        )

    def carries(way, s, h):
        return s > 0 or h == way

    for s in range(half_ring):
        for h in range(2):
            for way in range(2):
                hh = h if way == 0 else 1 - h
                if not carries(way, s, hh):
                    continue
                if s == 0:
                    pair_sum(hh)
                if s > 0 and carries(way, s - 1, hh):
                    reduce_copy(way, s - 1, hh).wait_recv()
                    step = 1 - 2 * way
                    at = slot_at(pos + step * (half_ring - s), core)
                    cc = slice(hh * hw, (hh + 1) * hw)
                    part[at, :, cc] = (
                        part[at, :, cc].astype(F32)
                        + rbuf[way, s - 1, hh].astype(F32)
                    ).astype(BF16)
                go(reduce_copy(way, s, hh))
    for h in range(2):
        cc = slice(h * hw, (h + 1) * hw)
        own = part[mine, :, cc].astype(F32)
        for way in range(2):
            if carries(way, half_ring - 1, h):
                reduce_copy(way, half_ring - 1, h).wait_recv()
                own += rbuf[way, half_ring - 1, h].astype(F32)
        own = own * gate
        own_hi = own.astype(BF16)
        own_out[0:CAP, cc] = own_hi
        own_out[CAP : 2 * CAP, cc] = (own - own_hi.astype(F32)).astype(BF16)

    am_copy.wait()
    for copy in started:
        copy.wait_send()
    for d in range(1, n):
        dest = (me + d) % n
        for_owner(dest, lambda: to_owner(dest, me).wait_send())

    def drain():
        for d in range(1, n):
            to_reader((me + d) % n, me).wait_send()

    for_owner(me, drain)


def combine_kernel(am, sel, own, out):
    back = jnp.dot(sel[:, 0 : own.shape[0]], own[...], preferred_element_type=F32)
    out[...] = (am[...].astype(F32) + back).astype(BF16)


def solution(mesh):
    n = mesh.shape["seq"]

    def body(
        hid, gain, proj, bias, rate, mgain, fgain, router, routes, wg, wu, wd
    ):
        tok, width = hid.shape
        heads = bias.shape[0]
        lanes = width // heads
        cols = proj.shape[1]
        state = (cols - heads) // 2
        owners = min(n, heads)
        per = heads // owners
        chips = n // 2
        half_ring = chips // 2
        vm = pl.BlockSpec(memory_space=pltpu.VMEM)
        anyspec = pl.BlockSpec(memory_space=pl.ANY)
        dma = pltpu.SemaphoreType.DMA
        am, own, sel = pl.pallas_call(
            functools.partial(block_kernel, n),
            out_shape=[
                jax.ShapeDtypeStruct((tok, width), BF16),
                jax.ShapeDtypeStruct((2 * CAP, width), BF16),
                jax.ShapeDtypeStruct((tok, 128), BF16),
            ],
            in_specs=[vm] * 9 + [anyspec] * 3,
            out_specs=[anyspec, vm, vm],
            scratch_shapes=[
                pltpu.VMEM(wg.shape[::-1], BF16),
                pltpu.VMEM(wu.shape[::-1], BF16),
                pltpu.VMEM(wd.shape, BF16),
                pltpu.VMEM((tok, width), BF16),
                pltpu.VMEM((tok, width), F32),
                pltpu.VMEM((tok, width), BF16),
                pltpu.VMEM((CAP, width), F32),
                pltpu.VMEM((CAP, width), BF16),
                pltpu.VMEM((CAP, width), BF16),
                pltpu.VMEM((tok, 128), BF16),
                pltpu.VMEM((heads, tok), F32),
                pltpu.VMEM((heads, tok), F32),
                pltpu.VMEM((heads, tok), F32),
                pltpu.VMEM((state, tok), F32),
                pltpu.VMEM((tok, tok), F32),
                pltpu.VMEM((tok, cols), BF16),
                pltpu.VMEM((tok, cols), BF16),
                pltpu.VMEM((owners, state + 16, per * lanes), BF16),
                pltpu.VMEM((n, state + 16, per * lanes), BF16),
                pltpu.VMEM((n, state, per * lanes), BF16),
                pltpu.VMEM((owners, state, per * lanes), BF16),
                pltpu.VMEM((n, CAP, width), BF16),
                pltpu.VMEM((n, CAP, width), BF16),
                pltpu.VMEM((chips, CAP, width), BF16),
                pltpu.VMEM((2, half_ring, 2, CAP, width // 2), BF16),
                dma((3,)),
                dma,
                dma((n,)),
                dma((n,)),
                dma((n,)),
                dma((n,)),
                dma((2, half_ring, 2)),
                dma((2, half_ring, 2)),
                dma((2, half_ring + 1, 2)),
                dma((2, half_ring + 1, 2)),
                dma((2,)),
                dma((2,)),
                dma((2, half_ring, 2)),
                dma((2, half_ring, 2)),
            ],
            compiler_params=pltpu.CompilerParams(
                collective_id=0,
                has_side_effects=True,
                vmem_limit_bytes=60 * 1024 * 1024,
            ),
        )(
            hid,
            gain.reshape(1, width),
            proj.T,
            bias.reshape(1, heads),
            rate.reshape(1, heads),
            mgain.reshape(1, width),
            fgain.reshape(1, width),
            router.T,
            routes.T,
            wg.T,
            wu.T,
            wd,
        )
        block = width // 4
        return pl.pallas_call(
            combine_kernel,
            grid=(4,),
            out_shape=jax.ShapeDtypeStruct((tok, width), BF16),
            in_specs=[
                pl.BlockSpec((tok, block), lambda i: (0, i)),
                pl.BlockSpec((tok, 128), lambda i: (0, 0)),
                pl.BlockSpec((2 * CAP, block), lambda i: (0, i)),
            ],
            out_specs=pl.BlockSpec((tok, block), lambda i: (0, i)),
        )(am, sel, own)

    both = P(("docs", "seq"), None)
    in_specs = (
        both, P(), P(), P(), P(), P(), P(), P(), both,
        P(None, "seq"), P(None, "seq"), P("seq", None),
    )
    return jax.shard_map(
        body, mesh=mesh, in_specs=in_specs, out_specs=both, check_vma=False
    )
```

```python
import functools

import jax
import jax.numpy as jnp
from jax import lax
from jax.experimental import pallas as pl
from jax.experimental.pallas import tpu as pltpu
from jax.sharding import PartitionSpec as P

CAP = 16
CUTS = 4
EPS = 1e-05
HI = lax.Precision.HIGHEST
MESH = pl.DeviceIdType.MESH
F32 = jnp.float32
BF16 = jnp.bfloat16


def remote(src, dst, send, recv, target):
    return pltpu.make_async_remote_copy(
        src_ref=src,
        dst_ref=dst,
        send_sem=send,
        recv_sem=recv,
        device_id={"seq": target},
        device_id_type=MESH,
    )


def across_last(a, b):
    return lax.dot_general(a, b, (((1,), (1,)), ((), ())), preferred_element_type=F32)


def iota(shape, dim):
    return lax.broadcasted_iota(jnp.int32, shape, dim)


def block_kernel(
    n,
    hid,
    gain,
    proj,
    bias,
    rate,
    mgain,
    fgain,
    router,
    routes,
    wg_hbm,
    wu_hbm,
    wd_hbm,
    am_out,
    own_out,
    sel_out,
    wg,
    wu,
    wd,
    xn,
    within,
    am,
    wsel,
    hsel,
    ysel,
    cum3,
    cumt,
    dtt,
    tet,
    bt,
    crossm,
    phi,
    plo,
    msg,
    inbox,
    scan_out,
    ent,
    gath,
    part,
    prt,
    rbuf,
    w_sem,
    am_sem,
    a_send,
    a_recv,
    b_send,
    b_recv,
    g_send,
    g_recv,
    d_send,
    d_recv,
    p_send,
    p_recv,
    r_send,
    r_recv,
):
    tok, width = hid.shape
    heads = bias.shape[1]
    lanes = width // heads
    state = (proj.shape[0] - heads) // 2
    owners = msg.shape[0]
    per = heads // owners
    chips = n // 2
    half_ring = chips // 2
    hw = width // CUTS
    near = CUTS // 2
    me = lax.axis_index("seq")
    core = me % 2
    chip = me // 2
    odd = chip % 2
    pos = (1 - odd) * (chip // 2) + odd * (chips - 1 - chip // 2)

    def device_at(place):
        place = (place + 2 * chips) % chips
        high = place // half_ring
        held = (1 - high) * (2 * place) + high * (2 * (chips - 1 - place) + 1)
        return held * 2 + core

    def slot_at(place, which):
        return which * chips + (place + 2 * chips) % chips

    partner = me + 1 - 2 * core

    barrier = pltpu.get_barrier_semaphore()
    for d in range(1, n):
        pl.semaphore_signal(
            barrier, inc=1, device_id={"seq": (me + d) % n}, device_id_type=MESH
        )

    loads = [
        pltpu.make_async_copy(a, b, w_sem.at[k])
        for k, (a, b) in enumerate(((wg_hbm, wg), (wu_hbm, wu), (wd_hbm, wd)))
    ]
    for load in loads:
        load.start()

    def norm_rows(i, _):
        rows = pl.ds(pl.multiple_of(i * 16, 16), 16)
        x = hid[rows, :].astype(F32)
        ms = jnp.mean(x * x, axis=-1, keepdims=True)
        xn[rows, :] = (x * lax.rsqrt(ms + EPS) * gain[...]).astype(BF16)
        return 0

    lax.fori_loop(0, tok // 16, norm_rows, 0)

    p = across_last(xn[...], proj[...])
    p_hi = p.astype(BF16)
    phi[...] = p_hi
    plo[...] = (p - p_hi.astype(F32)).astype(BF16)
    pt = p.T
    b_t = pt[0:state]
    eye = iota((heads, heads), 0) == iota((heads, heads), 1)
    bias_col = jnp.sum(jnp.where(eye, bias[...], 0.0), axis=1, keepdims=True)
    rate_col = jnp.sum(jnp.where(eye, rate[...], 0.0), axis=1, keepdims=True)
    v = pt[2 * state :] + bias_col
    dt = jnp.maximum(v, 0.0) + jnp.log(1.0 + jnp.exp(-jnp.abs(v)))
    upper = (iota((tok, tok), 0) <= iota((tok, tok), 1)).astype(F32)
    c_t = jnp.dot(-dt * rate_col, upper, precision=HI, preferred_element_type=F32)
    bt[...] = b_t
    dtt[...] = dt
    cumt[...] = c_t
    tet[...] = jnp.exp(c_t[:, tok - 1 : tok] - c_t) * dt
    c1 = c_t.astype(BF16).astype(F32)
    c2 = (c_t - c1).astype(BF16).astype(F32)
    c3 = c_t - c1 - c2
    pad = jnp.zeros((128 - 3 * heads, tok), F32)
    cum3[...] = jnp.concatenate([c1, c2, c3, pad], axis=0).T.astype(BF16)

    def spread(h):
        row = iota((128, lanes), 0)
        pick = ((row % heads) == h) & (row < 3 * heads)
        return jnp.where(pick, 1.0, 0.0).astype(BF16)

    def state_head(h, _):
        cols = pl.ds(pl.multiple_of(h * lanes, lanes), lanes)
        inner = pl.ds(pl.multiple_of((h % per) * lanes, lanes), lanes)
        sw = (bt[...] * tet[pl.ds(h, 1), :]).astype(BF16)
        s = jnp.dot(sw, xn[:, cols], preferred_element_type=F32)
        msg[h // per, 0:state, inner] = s.astype(BF16)
        last = jnp.dot(cum3[tok - 16 : tok, :], spread(h), preferred_element_type=F32)
        d = jnp.exp(last[15:16, :])
        d_hi = d.astype(BF16).astype(F32)
        row = iota((16, lanes), 0)
        packed = jnp.where(row == 0, d_hi, jnp.where(row == 1, d - d_hi, 0.0))
        msg[h // per, state : state + 16, inner] = packed.astype(BF16)
        return 0

    lax.fori_loop(0, heads, state_head, 0)

    pl.semaphore_wait(barrier, n - 1)

    def to_owner(owner, source):
        return remote(
            msg.at[owner], inbox.at[source], a_send.at[owner], a_recv.at[source], owner
        )

    def to_reader(reader, source):
        return remote(
            scan_out.at[reader],
            ent.at[source],
            b_send.at[reader],
            b_recv.at[source],
            reader,
        )

    every = owners == n

    def for_owner(index, run):
        if every:
            run()
        else:
            pl.when(index < owners)(run)

    for d in range(1, n):
        dest = (me + d) % n
        for_owner(dest, lambda: to_owner(dest, me).start())

    z = jnp.concatenate(
        [
            jnp.zeros((state, tok), F32),
            bt[...],
            jnp.zeros((p.shape[1] - 2 * state, tok), F32),
        ],
        axis=0,
    )
    cross = jnp.dot(p, z, precision=HI, preferred_element_type=F32)
    crossm[...] = jnp.where(iota((tok, tok), 0) >= iota((tok, tok), 1), cross, 0.0)

    r0 = routes[0:1, :]
    r1 = routes[1:2, :]
    hit = jnp.where((r0 == 0) | (r1 == 0), 1.0, 0.0)
    other = jnp.where(r0 == 0, r1, r0).astype(F32)
    wide = jnp.broadcast_to(hit, (CAP, tok))
    rank = jnp.dot(
        wide.astype(BF16), upper.astype(BF16), preferred_element_type=F32
    )
    sel_f = jnp.where((rank - 1.0).astype(jnp.int32) == iota((CAP, tok), 0), wide, 0.0)
    other_sel = jnp.sum(sel_f * other, axis=1, keepdims=True)
    sel = sel_f.astype(BF16)
    blank = jnp.zeros((128 - 2 * CAP, tok), F32)
    sel_out[...] = jnp.concatenate([sel_f, sel_f, blank], axis=0).T.astype(BF16)

    def pick(value):
        return jnp.dot(sel, value, preferred_element_type=F32).astype(BF16)

    hsel[...] = pick(hid[...])
    phi_sel = pick(phi[...])
    plo_sel = pick(plo[...])
    cum_sel = pick(cum3[...])

    mid = tok // 2

    def within_head(h, _):
        cols = pl.ds(pl.multiple_of(h * lanes, lanes), lanes)
        ch = jnp.dot(cum3[...], spread(h), preferred_element_type=F32)
        crow = cumt[pl.ds(h, 1), :]
        drow = dtt[pl.ds(h, 1), :]
        chosen = None
        for k in range(2):
            rows = slice(k * mid, (k + 1) * mid)
            total = None
            for j in range(k + 1):
                over = slice(j * mid, (j + 1) * mid)
                gap = ch[rows, :] - crow[:, over]
                w = crossm[rows, over] * jnp.exp(jnp.minimum(gap, 0.0)) * drow[:, over]
                term = jnp.dot(
                    w.astype(BF16), xn[over, cols], preferred_element_type=F32
                )
                total = term if total is None else total + term
            within[rows, cols] = total
            top = total.astype(BF16)
            low = (total - top.astype(F32)).astype(BF16)
            got = jnp.dot(
                sel[:, rows], top, preferred_element_type=F32
            ) + jnp.dot(sel[:, rows], low, preferred_element_type=F32)
            chosen = got if chosen is None else chosen + got
        wsel[:, cols] = chosen
        return 0

    lax.fori_loop(0, heads // 2, within_head, 0)

    def scan_all():
        inbox[me] = msg[me]
        for d in range(1, n):
            to_owner(0, (me + d) % n).wait_recv()
        running = jnp.zeros((state, per * lanes), F32)
        for j in range(n):
            scan_out[j] = running.astype(BF16)
            decay = (
                inbox[j, state : state + 1, :].astype(F32)
                + inbox[j, state + 1 : state + 2, :].astype(F32)
            )
            running = decay * running + inbox[j, 0:state, :].astype(F32)
        ent[me] = scan_out[me]
        for d in range(1, n):
            dest = (me + d) % n
            to_reader(dest, me).start()

    for_owner(me, scan_all)

    lax.fori_loop(heads // 2, heads, within_head, 0)

    for d in range(1, n):
        source = (me + d) % n
        for_owner(source, lambda: to_reader(0, source).wait_recv())

    def mixed(h, c_hi, c_lo, cum, inside, base):
        cols = pl.ds(pl.multiple_of(h * lanes, lanes), lanes)
        inner = pl.ds(pl.multiple_of((h % per) * lanes, lanes), lanes)
        e = ent[h // per, :, inner]
        zero = jnp.zeros((state, lanes), BF16)
        rest = jnp.zeros((phi.shape[1] - 2 * state, lanes), BF16)
        ez = jnp.concatenate([zero, e, rest], axis=0)
        carried = jnp.dot(c_hi, ez, preferred_element_type=F32) + jnp.dot(
            c_lo, ez, preferred_element_type=F32
        )
        ch = jnp.dot(cum, spread(h), preferred_element_type=F32)
        o = inside[:, cols] + jnp.exp(ch) * carried
        ms = jnp.mean(o * o, axis=-1, keepdims=True)
        y = base[:, cols].astype(F32) + o * lax.rsqrt(ms + EPS) * mgain[:, cols]
        return y.astype(BF16)

    def mix_chosen(i, _):
        for k in range(4):
            h = i * 4 + k
            cols = pl.ds(pl.multiple_of(h * lanes, lanes), lanes)
            ysel[:, cols] = mixed(h, phi_sel, plo_sel, cum_sel, wsel, hsel)
        return 0

    lax.fori_loop(0, heads // 4, mix_chosen, 0)

    x = ysel[...].astype(F32)
    ms = jnp.mean(x * x, axis=-1, keepdims=True)
    chosen_in = (x * lax.rsqrt(ms + EPS) * fgain[...]).astype(BF16)
    mine = slot_at(pos, core)
    gath[mine] = chosen_in

    def mix_head(h, _):
        cols = pl.ds(pl.multiple_of(h * lanes, lanes), lanes)
        am[:, cols] = mixed(h, phi[...], plo[...], cum3[...], within, hid)
        return 0

    def cut(h):
        return pl.ds(h * hw, hw)

    def ring(way, s, h, place):
        step = 1 - 2 * way
        block = gath.at[slot_at(place, core), :, cut(h)]
        return remote(
            block,
            block,
            g_send.at[way, s, h],
            g_recv.at[way, s, h],
            device_at(pos + step),
        )

    def across(way, s, h, place, which):
        block = gath.at[slot_at(place, which), :, cut(h)]
        return remote(
            block, block, d_send.at[way, s, h], d_recv.at[way, s, h], partner
        )

    started = []

    def go(copy):
        copy.start()
        started.append(copy)

    def used(way, s, h):
        return s < half_ring - 1 or h // near == way

    for h in range(CUTS):
        for way in range(2):
            hh = (h + near * way) % CUTS
            if used(way, 0, hh):
                go(ring(way, 0, hh, pos))
    def own_across(h, slot):
        block = gath.at[slot, :, cut(h)]
        return remote(
            block,
            block,
            d_send.at[0, half_ring, h],
            d_recv.at[0, half_ring, h],
            partner,
        )

    for h in range(CUTS):
        go(own_across(h, mine))

    logits = across_last(chosen_in, router[...])
    picked = jnp.sum(
        jnp.where(iota(logits.shape, 1) == other_sel.astype(jnp.int32), logits, 0.0),
        axis=1,
        keepdims=True,
    )
    gate = 1.0 / (1.0 + jnp.exp(picked - logits[:, 0:1]))

    pieces = CUTS * half_ring
    done = 0

    for s in range(half_ring):
        for h in range(CUTS):
            for way in range(2):
                hh = (h + near * way) % CUTS
                if not used(way, s, hh):
                    continue
                step = 1 - 2 * way
                place = pos - step * (1 + s)
                ring(way, s, hh, place).wait_recv()
                if s + 1 < half_ring and used(way, s + 1, hh):
                    go(ring(way, s + 1, hh, place))
                go(across(way, s, hh, place, core))
            upto = (CUTS * s + h + 1) * heads // pieces
            lax.fori_loop(done, upto, mix_head, 0)
            done = upto
    am_copy = pltpu.make_async_copy(am, am_out, am_sem)
    am_copy.start()
    for h in range(CUTS):
        own_across(h, slot_at(pos, 1 - core)).wait_recv()
    for s in range(half_ring):
        for way in range(2):
            for h in range(CUTS):
                if used(way, s, h):
                    step = 1 - 2 * way
                    across(way, s, h, pos - step * (1 + s), 1 - core).wait_recv()

    for load in loads:
        load.wait()
    rows_all = n * CAP
    x_all = gath[...].reshape(rows_all, width)
    g = across_last(x_all, wg[...])
    u = across_last(x_all, wu[...])
    hidden = (g / (1.0 + jnp.exp(-g)) * u).astype(BF16)

    def swap(h):
        return remote(
            part.at[pl.ds((1 - core) * chips, chips), :, cut(h)],
            prt.at[:, :, cut(h)],
            p_send.at[h],
            p_recv.at[h],
            partner,
        )

    for k in range(CUTS):
        h = (k // 2) + near * (k % 2)
        c = slice(h * hw, (h + 1) * hw)
        part[:, :, c] = (
            jnp.dot(hidden, wd[:, c], preferred_element_type=F32)
            .astype(BF16)
            .reshape(n, CAP, hw)
        )
        go(swap(h))

    def pair_sum(h):
        swap(h).wait_recv()
        cc = slice(h * hw, (h + 1) * hw)

        def one(i, _):
            at = core * chips + i
            part[at, :, cc] = (
                part[at, :, cc].astype(F32) + prt[i, :, cc].astype(F32)
            ).astype(BF16)
            return 0

        lax.fori_loop(0, chips, one, 0)

    def reduce_copy(way, s, h):
        step = 1 - 2 * way
        place = pos + step * (half_ring - s)
        return remote(
            part.at[slot_at(place, core), :, cut(h)],
            rbuf.at[way, s, h],
            r_send.at[way, s, h],
            r_recv.at[way, s, h],
            device_at(pos + step),
        )

    def carries(way, s, h):
        return s > 0 or h // near == way

    for s in range(half_ring):
        for h in range(CUTS):
            for way in range(2):
                hh = (h + near * way) % CUTS
                if not carries(way, s, hh):
                    continue
                if s == 0:
                    pair_sum(hh)
                if s > 0 and carries(way, s - 1, hh):
                    reduce_copy(way, s - 1, hh).wait_recv()
                    step = 1 - 2 * way
                    at = slot_at(pos + step * (half_ring - s), core)
                    cc = slice(hh * hw, (hh + 1) * hw)
                    part[at, :, cc] = (
                        part[at, :, cc].astype(F32)
                        + rbuf[way, s - 1, hh].astype(F32)
                    ).astype(BF16)
                go(reduce_copy(way, s, hh))
    for h in range(CUTS):
        cc = slice(h * hw, (h + 1) * hw)
        own = part[mine, :, cc].astype(F32)
        for way in range(2):
            if carries(way, half_ring - 1, h):
                reduce_copy(way, half_ring - 1, h).wait_recv()
                own += rbuf[way, half_ring - 1, h].astype(F32)
        own = own * gate
        own_hi = own.astype(BF16)
        own_out[0:CAP, cc] = own_hi
        own_out[CAP : 2 * CAP, cc] = (own - own_hi.astype(F32)).astype(BF16)

    am_copy.wait()
    for copy in started:
        copy.wait_send()
    for d in range(1, n):
        dest = (me + d) % n
        for_owner(dest, lambda: to_owner(dest, me).wait_send())

    def drain():
        for d in range(1, n):
            to_reader((me + d) % n, me).wait_send()

    for_owner(me, drain)


def combine_kernel(am, sel, own, out):
    back = jnp.dot(sel[:, 0 : own.shape[0]], own[...], preferred_element_type=F32)
    out[...] = (am[...].astype(F32) + back).astype(BF16)


def solution(mesh):
    n = mesh.shape["seq"]

    def body(
        hid, gain, proj, bias, rate, mgain, fgain, router, routes, wg, wu, wd
    ):
        tok, width = hid.shape
        heads = bias.shape[0]
        lanes = width // heads
        cols = proj.shape[1]
        state = (cols - heads) // 2
        owners = min(n, heads)
        per = heads // owners
        chips = n // 2
        half_ring = chips // 2
        vm = pl.BlockSpec(memory_space=pltpu.VMEM)
        anyspec = pl.BlockSpec(memory_space=pl.ANY)
        dma = pltpu.SemaphoreType.DMA
        am, own, sel = pl.pallas_call(
            functools.partial(block_kernel, n),
            out_shape=[
                jax.ShapeDtypeStruct((tok, width), BF16),
                jax.ShapeDtypeStruct((2 * CAP, width), BF16),
                jax.ShapeDtypeStruct((tok, 128), BF16),
            ],
            in_specs=[vm] * 9 + [anyspec] * 3,
            out_specs=[anyspec, vm, vm],
            scratch_shapes=[
                pltpu.VMEM(wg.shape[::-1], BF16),
                pltpu.VMEM(wu.shape[::-1], BF16),
                pltpu.VMEM(wd.shape, BF16),
                pltpu.VMEM((tok, width), BF16),
                pltpu.VMEM((tok, width), F32),
                pltpu.VMEM((tok, width), BF16),
                pltpu.VMEM((CAP, width), F32),
                pltpu.VMEM((CAP, width), BF16),
                pltpu.VMEM((CAP, width), BF16),
                pltpu.VMEM((tok, 128), BF16),
                pltpu.VMEM((heads, tok), F32),
                pltpu.VMEM((heads, tok), F32),
                pltpu.VMEM((heads, tok), F32),
                pltpu.VMEM((state, tok), F32),
                pltpu.VMEM((tok, tok), F32),
                pltpu.VMEM((tok, cols), BF16),
                pltpu.VMEM((tok, cols), BF16),
                pltpu.VMEM((owners, state + 16, per * lanes), BF16),
                pltpu.VMEM((n, state + 16, per * lanes), BF16),
                pltpu.VMEM((n, state, per * lanes), BF16),
                pltpu.VMEM((owners, state, per * lanes), BF16),
                pltpu.VMEM((n, CAP, width), BF16),
                pltpu.VMEM((n, CAP, width), BF16),
                pltpu.VMEM((chips, CAP, width), BF16),
                pltpu.VMEM((2, half_ring, CUTS, CAP, width // CUTS), BF16),
                dma((3,)),
                dma,
                dma((n,)),
                dma((n,)),
                dma((n,)),
                dma((n,)),
                dma((2, half_ring, CUTS)),
                dma((2, half_ring, CUTS)),
                dma((2, half_ring + 1, CUTS)),
                dma((2, half_ring + 1, CUTS)),
                dma((CUTS,)),
                dma((CUTS,)),
                dma((2, half_ring, CUTS)),
                dma((2, half_ring, CUTS)),
            ],
            compiler_params=pltpu.CompilerParams(
                collective_id=0,
                has_side_effects=True,
                vmem_limit_bytes=60 * 1024 * 1024,
            ),
        )(
            hid,
            gain.reshape(1, width),
            proj.T,
            bias.reshape(1, heads),
            rate.reshape(1, heads),
            mgain.reshape(1, width),
            fgain.reshape(1, width),
            router.T,
            routes.T,
            wg.T,
            wu.T,
            wd,
        )
        block = width // 8
        return pl.pallas_call(
            combine_kernel,
            grid=(8,),
            out_shape=jax.ShapeDtypeStruct((tok, width), BF16),
            in_specs=[
                pl.BlockSpec((tok, block), lambda i: (0, i)),
                pl.BlockSpec((tok, 128), lambda i: (0, 0)),
                pl.BlockSpec((2 * CAP, block), lambda i: (0, i)),
            ],
            out_specs=pl.BlockSpec((tok, block), lambda i: (0, i)),
        )(am, sel, own)

    both = P(("docs", "seq"), None)
    in_specs = (
        both, P(), P(), P(), P(), P(), P(), P(), both,
        P(None, "seq"), P(None, "seq"), P("seq", None),
    )
    return jax.shard_map(
        body, mesh=mesh, in_specs=in_specs, out_specs=both, check_vma=False
    )
```
